32 devices in a mesh: bits: 16 (over z, y, x), docs: 2 (over core).
Axes of the slice: x: 2, y: 2, z: 4, core: 2. Of those that a mesh axis runs over, the one named last changes fastest.
Arguments:
- positions: int32 [1024, 4096], P(('bits', 'docs')), may hold values from 0 to 4095
- element_weights: float32 [1024, 1024], P(('bits', 'docs')), may hold values from 0.25 to 4
- set_sizes: int32 [1024], P(('bits', 'docs')), may hold values from 256 to 1024, as said below
- bit_weights: bfloat16 [4096], replicated, may hold values from 0.25 to 4
- candidates: int32 [2, 16, 16], P('docs'), may hold values from 0 to 63, as said below
Outputs:
- scores: float32 [2, 16, 128, 64], P('docs', 'bits')
The draws below stay inside these ranges and needn't reach their ends.
Inputs may be any that keep to these rules, and one draw needn't show every extreme that they name: `set_sizes`: one document in every draw has exactly 1024 elements. `candidates`: the 16 row tiles named for one block are distinct. `positions`: entries of a row beyond its first 4 * set_sizes are not part of the filter.
All inputs are finite; a program needn't handle non-finite values.
Results may differ from the reference program's by a relative error of at most 0.0012.
Values may be sent and summed in bfloat16 or wider, within the bound.
A program may use at most 64 MiB of HBM per device.

```python
import math
import jax
import jax.numpy as jnp
import numpy as np
from jax import lax

FILTER_BITS = 4096
HASHES = 4
ELEMS = 1024
TILE = 8
CAND = 16
PMAX = 4096
DOCS = 1024
ROW_GROUPS = 2
COL_BLOCKS = 16
ROW_HALF = 512
COLS = 64
RTILES = 64


def draw_set_sizes(key, part):
    levels = 64
    ladder = np.floor(ELEMS * 4.0 ** ((np.arange(levels) - (levels - 1)) / (levels - 1.0)))
    ladder = np.maximum(ladder, 1).astype(np.int32)
    pick_key, doc_key = jax.random.split(jax.random.fold_in(key, 11))
    picked = jax.random.randint(pick_key, (DOCS,), 0, levels)
    set_count = jnp.asarray(ladder)[picked]
    chosen_doc = jax.random.randint(doc_key, (), 0, DOCS)
    return set_count.at[chosen_doc].set(ELEMS).astype(jnp.int32)


def draw_candidates(key, part):
    block_keys = jax.random.split(jax.random.fold_in(key, 23), ROW_GROUPS * COL_BLOCKS)
    picked = jax.vmap(lambda sub_key: jax.random.permutation(sub_key, RTILES)[:CAND])(block_keys)
    return picked.reshape(ROW_GROUPS, COL_BLOCKS, CAND).astype(jnp.int32)


def place_ends(entries, stream_key, least, high):
    place = [jax.random.randint(jax.random.fold_in(stream_key, axis), (), 0, length) for axis, length in enumerate(entries.shape)]
    main_axis = entries.shape.index(max(entries.shape))
    beside = place[:main_axis] + [(place[main_axis] + 1) % entries.shape[main_axis]] + place[main_axis + 1:]
    return entries.at[tuple(place)].set(least).at[tuple(beside)].set(high)


def block_levels(rng, extent, pieces, least, top_value):
    factor_of = 1.0
    for dim, shards_of in pieces:
        steps = jax.random.uniform(jax.random.fold_in(jax.random.fold_in(rng, 6), dim), (shards_of,), jnp.float32, least / len(pieces), top_value / len(pieces))
        factor_of = factor_of * jnp.repeat(jnp.exp(steps), extent[dim] // shards_of).reshape((-1,) + (1,) * (len(extent) - 1 - dim))
    return factor_of


def setup_inputs(seed: int = 0) -> dict:
    key_of = jax.random.split(jax.random.key(seed), 6)
    positions = place_ends(jax.random.randint(key_of[0], (DOCS, PMAX), 0, FILTER_BITS), jax.random.fold_in(key_of[0], 1), 0, FILTER_BITS - 1).astype(jnp.int32)
    element_weights = jnp.clip(jnp.exp(math.log(4.0) - 2.7725887 * jax.random.uniform(key_of[1], (DOCS, ELEMS), jnp.float32) ** block_levels(key_of[1], (DOCS, ELEMS), ((0, 32),), -0.2, 0.2)), 0.25, 4.0)
    set_sizes = draw_set_sizes(jax.random.fold_in(key_of[5], 71), 0)
    bit_weights = jnp.clip(jnp.exp(jax.random.uniform(key_of[3], (FILTER_BITS,), jnp.float32, math.log(0.25), math.log(4.0))), 0.25, 4.0).astype(jnp.bfloat16)
    candidates = draw_candidates(jax.random.fold_in(key_of[5], 71), 0)
    return {"positions": positions, "element_weights": element_weights, "set_sizes": set_sizes, "bit_weights": bit_weights, "candidates": candidates}


def build_filter(positions, element_weights, set_sizes):
    doc_count, slot_count = positions.shape
    slot_index = jnp.arange(slot_count, dtype=jnp.int32)
    usable = slot_index[None, :] < HASHES * set_sizes[:, None]
    target = jnp.where(usable, positions, FILTER_BITS).astype(jnp.int32)
    row_index = jnp.broadcast_to(jnp.arange(doc_count, dtype=jnp.int32)[:, None], positions.shape)
    slot_weights = jnp.repeat(element_weights.astype(jnp.float32), HASHES, axis=1)
    summed = jnp.zeros((doc_count, FILTER_BITS), jnp.float32).at[row_index, target].add(slot_weights, mode="drop")
    return summed.astype(jnp.bfloat16)


def reference(positions, element_weights, set_sizes, bit_weights, candidates):
    cell_matrix = build_filter(positions, element_weights, set_sizes)
    weighted_all = cell_matrix * bit_weights
    popcount = jnp.sum(weighted_all.astype(jnp.float32) * cell_matrix.astype(jnp.float32), axis=1)
    offsets = jnp.arange(TILE, dtype=jnp.int32)
    starts = (jnp.arange(ROW_GROUPS, dtype=jnp.int32) * ROW_HALF)[:, None, None, None]
    row_docs = (starts + candidates[:, :, :, None] * TILE + offsets).reshape(ROW_GROUPS, COL_BLOCKS, CAND * TILE)
    row_docs = row_docs.astype(jnp.int32)
    columns = cell_matrix.reshape(COL_BLOCKS, COLS, FILTER_BITS).astype(jnp.float32)

    def one_group(group_rows):
        weighted = weighted_all[group_rows].astype(jnp.float32)
        return jnp.einsum("dcb,dkb->dck", weighted, columns, precision=lax.Precision.HIGHEST)

    shared = lax.map(one_group, row_docs)
    pop_rows = popcount[row_docs][..., None]
    pop_cols = popcount.reshape(COL_BLOCKS, COLS)[None, :, None, :]
    size_float = set_sizes.astype(jnp.float32)
    size_rows = size_float[row_docs][..., None]
    size_cols = size_float.reshape(COL_BLOCKS, COLS)[None, :, None, :]
    ratio = shared / (pop_rows + pop_cols - shared)
    return ratio * (size_rows + size_cols) / ((1.0 + ratio) * jnp.minimum(size_rows, size_cols))
```

```python
import functools
import math

import jax
import jax.numpy as jnp
from jax import lax
from jax.experimental import pallas as pl
from jax.experimental.pallas import tpu as pltpu
from jax.sharding import PartitionSpec as P

FILTER_BITS = 4096
HASHES = 4
TILE = 8
LANES = 128
CHUNK = 512
STEPS = (0, 127, 126, 3, 122, 6, 125, 8)
MESH = pl.DeviceIdType.MESH


def build_filter(positions, element_weights, set_sizes):
    doc_count, slot_count = positions.shape
    elem_count = element_weights.shape[1]
    low_cells = 64
    high_cells = FILTER_BITS // low_cells
    slot_index = jnp.arange(slot_count, dtype=jnp.int32)
    usable = slot_index[None, :] < HASHES * set_sizes[:, None]
    spread = jnp.broadcast_to(element_weights[:, :, None], (doc_count, elem_count, HASHES)).reshape(
        doc_count, slot_count
    )
    slot_weights = jnp.where(usable, spread, 0.0)
    upper = slot_weights.astype(jnp.bfloat16)
    remain = slot_weights - upper.astype(jnp.float32)
    middle = remain.astype(jnp.bfloat16)
    lower = (remain - middle.astype(jnp.float32)).astype(jnp.bfloat16)
    weight_parts = jnp.stack([upper, middle, lower], axis=1)
    high_index = positions // low_cells
    low_index = positions - high_index * low_cells
    group = math.gcd(doc_count, 8)

    def one_group(inputs):
        part_block, high_block, low_block = inputs
        high_onehot = (high_block[:, :, None] == jnp.arange(high_cells, dtype=jnp.int32)).astype(
            jnp.bfloat16
        )
        low_onehot = (low_block[:, :, None] == jnp.arange(low_cells, dtype=jnp.int32)).astype(
            jnp.bfloat16
        )
        left = part_block[:, :, :, None] * high_onehot[:, None, :, :]
        summed = jnp.einsum("dcph,dpl->dhl", left, low_onehot, preferred_element_type=jnp.float32)
        return summed.reshape(group, FILTER_BITS)

    grouped = lax.map(
        one_group,
        (
            weight_parts.reshape(doc_count // group, group, 3, slot_count),
            high_index.reshape(doc_count // group, group, slot_count),
            low_index.reshape(doc_count // group, group, slot_count),
        ),
    )
    return grouped.reshape(doc_count, FILTER_BITS).astype(jnp.bfloat16)


def weighted_pop(cells, weights):
    weighted = cells * weights
    return jnp.sum(weighted.astype(jnp.float32) * cells.astype(jnp.float32), axis=1)


def estimate(shared, pop_rows, pop_cols, size_rows, size_cols):
    union_weight = pop_rows[:, None] + pop_cols[None, :] - shared
    ratio = shared / union_weight
    smaller = jnp.minimum(size_rows[:, None], size_cols[None, :])
    return ratio * (size_rows[:, None] + size_cols[None, :]) / ((1.0 + ratio) * smaller)


def pick_tiles(slice_cells, tile_choice, row_group, groups, row_half):
    width = slice_cells.shape[1]
    row_tiles = row_half // TILE
    tiles = slice_cells.reshape(groups, row_tiles, TILE * width)
    own_tiles = lax.dynamic_index_in_dim(tiles, row_group, 0, keepdims=False)
    onehot = (tile_choice[:, :, None] == jnp.arange(row_tiles, dtype=jnp.int32)).astype(
        jnp.bfloat16
    )
    picked = jnp.einsum("jcr,rw->jcw", onehot, own_tiles, preferred_element_type=jnp.float32)
    return picked.astype(jnp.bfloat16).reshape(
        tile_choice.shape[0], tile_choice.shape[1] * TILE, width
    )


def body(positions, element_weights, set_sizes, bit_weights, candidates):
    col_index = lax.axis_index("bits")
    row_group = lax.axis_index("docs")
    blocks = lax.axis_size("bits")
    groups = lax.axis_size("docs")
    doc_total = positions.shape[0] * blocks * groups
    row_half = doc_total // groups
    col_width = doc_total // blocks
    slot_count = candidates.shape[2] * TILE
    tile_offsets = jnp.arange(TILE, dtype=jnp.int32)
    own_cells = build_filter(positions, element_weights, set_sizes)
    local_pop = weighted_pop(own_cells, bit_weights)
    every_pop, size_float = (
        lax.all_gather(local_pop, ("bits", "docs"), axis=0, tiled=True),
        lax.all_gather(set_sizes.astype(jnp.float32), ("bits", "docs"), axis=0, tiled=True),
    )
    pair_cells = lax.all_gather(own_cells, "docs", axis=0, tiled=True)
    slice_cells = lax.all_to_all(pair_cells, "bits", split_axis=1, concat_axis=0, tiled=True)
    tile_rows = row_group * row_half + (candidates[0][:, :, None] * TILE + tile_offsets).reshape(
        blocks, slot_count
    )
    picked_cells = pick_tiles(slice_cells, candidates[0], row_group, groups, row_half)
    row_cells = lax.all_to_all(picked_cells, "bits", split_axis=0, concat_axis=2, tiled=True)[0]
    shared = lax.dot_general(
        row_cells * bit_weights,
        pair_cells,
        (((1,), (1,)), ((), ())),
        preferred_element_type=jnp.float32,
    )
    row_docs = lax.dynamic_index_in_dim(tile_rows, col_index, 0, keepdims=False)
    pop_rows = every_pop[row_docs]
    pop_cols = lax.dynamic_slice_in_dim(every_pop, col_index * col_width, col_width, 0)
    size_rows = size_float[row_docs]
    size_cols = lax.dynamic_slice_in_dim(size_float, col_index * col_width, col_width, 0)
    scores = estimate(shared, pop_rows, pop_cols, size_rows, size_cols)
    return scores.reshape(1, 1, slot_count, col_width)


NT = (((1,), (1,)), ((), ()))


def two_factors(value):
    best_a = value.astype(jnp.bfloat16).astype(jnp.float32)
    best_b = jnp.ones_like(value)
    best_e = jnp.abs(best_a - value)
    for step in STEPS[1:]:
        b = 1.0 + step / 128.0
        a = (value * (1.0 / b)).astype(jnp.bfloat16).astype(jnp.float32)
        e = jnp.abs(a * b - value)
        better = e < best_e
        best_a = jnp.where(better, a, best_a)
        best_b = jnp.where(better, b, best_b)
        best_e = jnp.where(better, e, best_e)
    return best_a, best_b


def fused_kernel(blocks, groups, cand_ref, sizes_ref, pos_ref, elem_ref, bw_ref, out_ref,
                 high_s, low_s, a_s, b_s, rows, outbox, stat_own, slab, stat, weighted, part, inbox,
                 send1, recv1, send1s, recv1s, send2, recv2, send2s, recv2s, send3, recv3):
    col, grp = lax.axis_index("bits"), lax.axis_index("docs")
    docs, slots = pos_ref.shape
    elems = elem_ref.shape[1]
    span = slab.shape[3]
    picks = cand_ref.shape[2]
    owners = blocks * groups
    near = docs // TILE
    me = col * groups + grp
    other = lax.rem(grp + 1, groups)
    half = LANES // 2
    highs = FILTER_BITS // half
    lines = FILTER_BITS // LANES

    barrier = pltpu.get_barrier_semaphore()
    for k in range(1, blocks):
        pl.semaphore_signal(barrier, inc=1, device_id=(lax.rem(col + k, blocks), grp), device_id_type=MESH)
    for k in range(1, groups):
        pl.semaphore_signal(barrier, inc=1, device_id=(col, lax.rem(grp + k, groups)), device_id_type=MESH)

    lane = lax.broadcasted_iota(jnp.int32, (docs, LANES), 1)
    sub = lax.broadcasted_iota(jnp.int32, (docs, LANES), 0)
    size_of = jnp.zeros((docs, LANES), jnp.int32)
    for d in range(docs):
        size_of = jnp.where(sub == d, sizes_ref[d], size_of)
    width = 2 * LANES
    wide = (lax.broadcasted_iota(jnp.int32, (width, HASHES * width), 1) // HASHES
            == lax.broadcasted_iota(jnp.int32, (width, HASHES * width), 0))
    wide = jnp.where(wide, 1.0, 0.0).astype(jnp.bfloat16)
    size_wide = jnp.concatenate([size_of] * (width // LANES), axis=1)
    lane_wide = lax.broadcasted_iota(jnp.int32, (docs, width), 1)
    for q in range(elems // width):
        value = elem_ref[:, q * width:(q + 1) * width]
        value = jnp.where(lane_wide + q * width < size_wide, value, 0.0)
        for place, part_of in zip((a_s, b_s), two_factors(value)):
            place[:, q * HASHES * width:(q + 1) * HASHES * width] = jnp.dot(
                part_of.astype(jnp.bfloat16), wide, preferred_element_type=jnp.float32)
    for q in range(slots // CHUNK):
        at = slice(q * CHUNK, (q + 1) * CHUNK)
        pos = pos_ref[:, at]
        high_s[:, at] = lax.shift_right_logical(pos, 6).astype(jnp.float32)
        low_s[:, at] = lax.bitwise_and(pos, half - 1).astype(jnp.float32)

    index = lax.broadcasted_iota(jnp.int32, (highs, LANES), 0)
    high_at = 2 * lax.rem(index, lines) + lax.div(index, lines)
    high_at = jnp.concatenate([high_at.astype(jnp.float32).astype(jnp.bfloat16)] * (CHUNK // LANES), axis=1)
    low_at = jnp.concatenate([index.astype(jnp.float32).astype(jnp.bfloat16)] * (CHUNK // LANES), axis=1)
    zero = jnp.zeros((half, CHUNK), jnp.bfloat16)

    def spread_row(ref, row, at):
        line = jnp.broadcast_to(ref[pl.ds(row, 1), at], (16, CHUNK)).astype(jnp.bfloat16)
        return jnp.concatenate([line] * (half // 16), axis=0)

    def remote(src, dst, send, recv, device):
        return pltpu.make_async_remote_copy(
            src_ref=src, dst_ref=dst, send_sem=send, recv_sem=recv, device_id=device, device_id_type=MESH)

    order = sorted(range(1, blocks), key=lambda k: -min(k, blocks - k))

    def first(q, k):
        to = lax.rem(col + k, blocks)
        return remote(outbox.at[q, to], slab.at[q, me], send1.at[q, k], recv1.at[q, k], (to, grp))

    def second(q, k):
        slot = lax.rem(col - k + blocks, blocks) * groups + grp
        source = slab.at[q, slot] if k else outbox.at[q, col]
        return remote(source, slab.at[q, slot], send2.at[q, k], recv2.at[q, k], (col, other))

    def first_stat(k):
        to = lax.rem(col + k, blocks)
        return remote(stat_own, stat.at[me], send1s.at[k], recv1s.at[k], (to, grp))

    def second_stat(k):
        slot = lax.rem(col - k + blocks, blocks) * groups + grp
        source = stat.at[slot] if k else stat_own
        return remote(source, stat.at[slot], send2s.at[k], recv2s.at[k], (col, other))

    def hand_on(q):
        for k in order[::-1]:
            first(q, k).wait_recv()
            second(q, k).start()

    def one_group(q, pops):
        for r in range(TILE):
            d = q * TILE + r
            total = jnp.zeros((highs, half), jnp.float32)
            for c in range(slots // CHUNK):
                at = slice(c * CHUNK, (c + 1) * CHUNK)
                left = jnp.where(spread_row(high_s, d, at) == high_at, spread_row(a_s, d, at), zero)
                right = jnp.where(spread_row(low_s, d, at) == low_at, spread_row(b_s, d, at), zero)
                total = total + lax.dot_general(left, right, NT, preferred_element_type=jnp.float32)
            rows[pl.ds(r, lines, stride=TILE), :] = jnp.concatenate([total[:lines], total[lines:]], axis=1)
        pop = jnp.zeros((TILE, LANES), jnp.float32)
        for h in range(lines):
            cells = rows[h * TILE:(h + 1) * TILE, :].astype(jnp.bfloat16)
            outbox[q, h * LANES // span, :, h * LANES % span:h * LANES % span + LANES] = cells
            full = cells.astype(jnp.float32)
            weight = bw_ref[h * LANES:(h + 1) * LANES].astype(jnp.float32).reshape(1, LANES)
            pop = pop + (full * weight).astype(jnp.bfloat16).astype(jnp.float32) * full
        pop = jnp.sum(pop, axis=1, keepdims=True)
        spot = lane[:TILE] == sub[:TILE] + q * TILE
        pops = pops + jnp.sum(jnp.where(spot, pop, 0.0), axis=0, keepdims=True)

        @pl.when(q == 0)
        def _():
            pl.semaphore_wait(barrier, blocks + groups - 2)

        for k in order:
            first(q, k).start()
        second(q, 0).start()
        slab[q, me] = outbox[q, col]

        @pl.when(q >= 2)
        def _():
            hand_on(q - 2)

        return pops

    pops = lax.fori_loop(0, near, one_group, jnp.zeros((1, LANES), jnp.float32))
    sizes = jnp.sum(jnp.where(lane == sub + docs, size_of.astype(jnp.float32), 0.0), axis=0, keepdims=True)
    stat_own[...] = pops + sizes
    for k in order:
        first_stat(k).start()
    second_stat(0).start()
    stat[me] = stat_own[...]
    for q in range(max(near - 2, 0), near):
        hand_on(q)
    for k in order[::-1]:
        first_stat(k).wait_recv()
        second_stat(k).start()
    for k in [0] + order[::-1]:
        for q in range(near):
            second(q, k).wait_recv()
        second_stat(k).wait_recv()

    bw = bw_ref[pl.ds(pl.multiple_of(col * span, span), span)].astype(jnp.float32).reshape(1, span)
    for o in range(owners // groups):
        for q in range(near):
            value = slab[q, grp * (owners // groups) + o].astype(jnp.float32) * bw
            weighted[o * near + q] = value.astype(jnp.bfloat16).astype(jnp.float32)

    third = []
    for k in order + [0]:
        block = lax.rem(col + k, blocks)
        tiles = [weighted[cand_ref[0, block, c]] for c in range(picks)]
        lines_in = jnp.concatenate(tiles, axis=0).astype(jnp.bfloat16)
        columns = jnp.concatenate(
            [slab[q, block * groups + o] for o in range(groups) for q in range(near)], axis=0)
        shared = lax.dot_general(columns, lines_in, NT, preferred_element_type=jnp.float32)
        if k:
            part[k] = shared.astype(part.dtype)
            copy = remote(part.at[k], inbox.at[k], send3.at[k], recv3.at[k], (block, grp))
            copy.start()
            third.append((k, copy))

    eight = lax.broadcasted_iota(jnp.int32, (TILE, LANES), 0)
    lanes = lax.broadcasted_iota(jnp.int32, (TILE, LANES), 1)
    pop_rows = jnp.zeros((TILE, LANES), jnp.float32)
    size_rows = jnp.zeros((TILE, LANES), jnp.float32)
    for c in range(picks):
        tile = cand_ref[0, col, c]
        line = stat[grp * (owners // groups) + lax.div(tile, near)]
        spot = lanes - lax.rem(tile, near) * TILE - eight
        pop = jnp.sum(jnp.where(spot == 0, line, 0.0), axis=1, keepdims=True)
        size = jnp.sum(jnp.where(spot == docs, line, 0.0), axis=1, keepdims=True)
        here = lanes == eight + c * TILE
        pop_rows = jnp.where(here, pop, pop_rows)
        size_rows = jnp.where(here, size, size_rows)
    pop_rows = jnp.sum(pop_rows, axis=0, keepdims=True)
    size_rows = jnp.sum(size_rows, axis=0, keepdims=True)
    mine = [stat[col * groups + o] for o in range(groups)]
    pop_cols = jnp.concatenate(
        [jnp.sum(jnp.where(lane == sub, line, 0.0), axis=1, keepdims=True) for line in mine], axis=0)
    size_cols = jnp.concatenate(
        [jnp.sum(jnp.where(lane == sub + docs, line, 0.0), axis=1, keepdims=True) for line in mine], axis=0)

    for k, copy in third[::-1]:
        copy.wait_recv()
        shared = shared + inbox[k].astype(jnp.float32)
    ratio = shared / (pop_rows + pop_cols - shared)
    out_ref[...] = ratio * (size_rows + size_cols) / ((1.0 + ratio) * jnp.minimum(size_rows, size_cols))
    for k, copy in third:
        copy.wait_send()
    for k in [0] + order:
        for q in range(near):
            if k:
                first(q, k).wait_send()
            second(q, k).wait_send()
        if k:
            first_stat(k).wait_send()
        second_stat(k).wait_send()


def fast_body(blocks, groups, positions, element_weights, set_sizes, bit_weights, candidates):
    docs, slots = positions.shape
    span = FILTER_BITS // blocks
    owners, near = blocks * groups, docs // TILE
    width, rows = docs * groups, candidates.shape[2] * TILE
    vmem, smem = pl.BlockSpec(memory_space=pltpu.VMEM), pl.BlockSpec(memory_space=pltpu.SMEM)
    one = lambda: pltpu.SemaphoreType.DMA((blocks,))
    many = lambda: pltpu.SemaphoreType.DMA((near, blocks))
    scores = pl.pallas_call(
        functools.partial(fused_kernel, blocks, groups),
        out_shape=jax.ShapeDtypeStruct((width, rows), jnp.float32),
        in_specs=[smem, smem, vmem, vmem, vmem],
        out_specs=vmem,
        scratch_shapes=[pltpu.VMEM((docs, slots), jnp.float32)] * 4 + [
            pltpu.VMEM((FILTER_BITS // LANES * TILE, LANES), jnp.float32),
            pltpu.VMEM((near, blocks, TILE, span), jnp.bfloat16),
            pltpu.VMEM((1, LANES), jnp.float32),
            pltpu.VMEM((near, owners, TILE, span), jnp.bfloat16),
            pltpu.VMEM((owners, 1, LANES), jnp.float32),
            pltpu.VMEM((docs * blocks // TILE, TILE, span), jnp.float32),
            pltpu.VMEM((blocks, width, rows), jnp.bfloat16),
            pltpu.VMEM((blocks, width, rows), jnp.bfloat16),
        ] + [many(), many(), one(), one(), many(), many(), one(), one(), one(), one()],
        compiler_params=pltpu.CompilerParams(collective_id=0, has_side_effects=True),
    )(candidates, set_sizes, positions, element_weights, bit_weights)
    return scores.T.reshape(1, 1, rows, width)


def solution(mesh):
    blocks, groups = mesh.shape["bits"], mesh.shape["docs"]
    fits = groups == 2 and FILTER_BITS % (blocks * LANES) == 0
    chosen = functools.partial(fast_body, blocks, groups) if fits else body
    return jax.shard_map(
        chosen,
        mesh=mesh,
        in_specs=(
            P(("bits", "docs"), None),
            P(("bits", "docs"), None),
            P(("bits", "docs")),
            P(),
            P("docs", None, None),
        ),
        out_specs=P("docs", "bits", None, None),
        check_vma=False,
    )
```

```python
import functools
import math

import jax
import jax.numpy as jnp
from jax import lax
from jax.experimental import pallas as pl
from jax.experimental.pallas import tpu as pltpu
from jax.sharding import PartitionSpec as P

FILTER_BITS = 4096
HASHES = 4
TILE = 8
LANES = 128
CHUNK = 512
STEPS = (0, 127, 126, 3, 122, 6, 125, 8)
MESH = pl.DeviceIdType.MESH


def build_filter(positions, element_weights, set_sizes):
    doc_count, slot_count = positions.shape
    elem_count = element_weights.shape[1]
    low_cells = 64
    high_cells = FILTER_BITS // low_cells
    slot_index = jnp.arange(slot_count, dtype=jnp.int32)
    usable = slot_index[None, :] < HASHES * set_sizes[:, None]
    spread = jnp.broadcast_to(element_weights[:, :, None], (doc_count, elem_count, HASHES)).reshape(
        doc_count, slot_count
    )
    slot_weights = jnp.where(usable, spread, 0.0)
    upper = slot_weights.astype(jnp.bfloat16)
    remain = slot_weights - upper.astype(jnp.float32)
    middle = remain.astype(jnp.bfloat16)
    lower = (remain - middle.astype(jnp.float32)).astype(jnp.bfloat16)
    weight_parts = jnp.stack([upper, middle, lower], axis=1)
    high_index = positions // low_cells
    low_index = positions - high_index * low_cells
    group = math.gcd(doc_count, 8)

    def one_group(inputs):
        part_block, high_block, low_block = inputs
        high_onehot = (high_block[:, :, None] == jnp.arange(high_cells, dtype=jnp.int32)).astype(
            jnp.bfloat16
        )
        low_onehot = (low_block[:, :, None] == jnp.arange(low_cells, dtype=jnp.int32)).astype(
            jnp.bfloat16
        )
        left = part_block[:, :, :, None] * high_onehot[:, None, :, :]
        summed = jnp.einsum("dcph,dpl->dhl", left, low_onehot, preferred_element_type=jnp.float32)
        return summed.reshape(group, FILTER_BITS)

    grouped = lax.map(
        one_group,
        (
            weight_parts.reshape(doc_count // group, group, 3, slot_count),
            high_index.reshape(doc_count // group, group, slot_count),
            low_index.reshape(doc_count // group, group, slot_count),
        ),
    )
    return grouped.reshape(doc_count, FILTER_BITS).astype(jnp.bfloat16)


def weighted_pop(cells, weights):
    weighted = cells * weights
    return jnp.sum(weighted.astype(jnp.float32) * cells.astype(jnp.float32), axis=1)


def estimate(shared, pop_rows, pop_cols, size_rows, size_cols):
    union_weight = pop_rows[:, None] + pop_cols[None, :] - shared
    ratio = shared / union_weight
    smaller = jnp.minimum(size_rows[:, None], size_cols[None, :])
    return ratio * (size_rows[:, None] + size_cols[None, :]) / ((1.0 + ratio) * smaller)


def pick_tiles(slice_cells, tile_choice, row_group, groups, row_half):
    width = slice_cells.shape[1]
    row_tiles = row_half // TILE
    tiles = slice_cells.reshape(groups, row_tiles, TILE * width)
    own_tiles = lax.dynamic_index_in_dim(tiles, row_group, 0, keepdims=False)
    onehot = (tile_choice[:, :, None] == jnp.arange(row_tiles, dtype=jnp.int32)).astype(
        jnp.bfloat16
    )
    picked = jnp.einsum("jcr,rw->jcw", onehot, own_tiles, preferred_element_type=jnp.float32)
    return picked.astype(jnp.bfloat16).reshape(
        tile_choice.shape[0], tile_choice.shape[1] * TILE, width
    )


def body(positions, element_weights, set_sizes, bit_weights, candidates):
    col_index = lax.axis_index("bits")
    row_group = lax.axis_index("docs")
    blocks = lax.axis_size("bits")
    groups = lax.axis_size("docs")
    doc_total = positions.shape[0] * blocks * groups
    row_half = doc_total // groups
    col_width = doc_total // blocks
    slot_count = candidates.shape[2] * TILE
    tile_offsets = jnp.arange(TILE, dtype=jnp.int32)
    own_cells = build_filter(positions, element_weights, set_sizes)
    local_pop = weighted_pop(own_cells, bit_weights)
    every_pop, size_float = (
        lax.all_gather(local_pop, ("bits", "docs"), axis=0, tiled=True),
        lax.all_gather(set_sizes.astype(jnp.float32), ("bits", "docs"), axis=0, tiled=True),
    )
    pair_cells = lax.all_gather(own_cells, "docs", axis=0, tiled=True)
    slice_cells = lax.all_to_all(pair_cells, "bits", split_axis=1, concat_axis=0, tiled=True)
    tile_rows = row_group * row_half + (candidates[0][:, :, None] * TILE + tile_offsets).reshape(
        blocks, slot_count
    )
    picked_cells = pick_tiles(slice_cells, candidates[0], row_group, groups, row_half)
    row_cells = lax.all_to_all(picked_cells, "bits", split_axis=0, concat_axis=2, tiled=True)[0]
    shared = lax.dot_general(
        row_cells * bit_weights,
        pair_cells,
        (((1,), (1,)), ((), ())),
        preferred_element_type=jnp.float32,
    )
    row_docs = lax.dynamic_index_in_dim(tile_rows, col_index, 0, keepdims=False)
    pop_rows = every_pop[row_docs]
    pop_cols = lax.dynamic_slice_in_dim(every_pop, col_index * col_width, col_width, 0)
    size_rows = size_float[row_docs]
    size_cols = lax.dynamic_slice_in_dim(size_float, col_index * col_width, col_width, 0)
    scores = estimate(shared, pop_rows, pop_cols, size_rows, size_cols)
    return scores.reshape(1, 1, slot_count, col_width)


NT = (((1,), (1,)), ((), ()))


def two_factors(value):
    best_a = value.astype(jnp.bfloat16).astype(jnp.float32)
    best_b = jnp.ones_like(value)
    best_e = jnp.abs(best_a - value)
    for step in STEPS[1:]:
        b = 1.0 + step / 128.0
        a = (value * (1.0 / b)).astype(jnp.bfloat16).astype(jnp.float32)
        e = jnp.abs(a * b - value)
        better = e < best_e
        best_a = jnp.where(better, a, best_a)
        best_b = jnp.where(better, b, best_b)
        best_e = jnp.where(better, e, best_e)
    return best_a, best_b


def fused_kernel(blocks, groups, cand_ref, sizes_ref, pos_ref, elem_ref, bw_ref, out_ref,
                 spread, rows, outbox, stat_own, slab, stat, weighted, part, inbox,
                 send1, recv1, send1s, recv1s, send2, recv2, send2s, recv2s, send3, recv3):
    col, grp = lax.axis_index("bits"), lax.axis_index("docs")
    docs, slots = pos_ref.shape
    elems = elem_ref.shape[1]
    span = slab.shape[4]
    picks = cand_ref.shape[2]
    near = docs // TILE
    other = 1 - grp
    half = LANES // 2
    highs = FILTER_BITS // half
    lines = FILTER_BITS // LANES
    peers = blocks - 1

    def shifted(k):
        return lax.bitwise_and(col + k, blocks - 1)

    barrier = pltpu.get_barrier_semaphore()
    for k in range(1, blocks):
        pl.semaphore_signal(barrier, inc=1, device_id=(shifted(k), grp), device_id_type=MESH)
    pl.semaphore_signal(barrier, inc=1, device_id=(col, other), device_id_type=MESH)

    lane = lax.broadcasted_iota(jnp.int32, (docs, LANES), 1)
    sub = lax.broadcasted_iota(jnp.int32, (docs, LANES), 0)
    lane8, sub8 = lane[:TILE], sub[:TILE]
    takes = [lax.div(lane8, HASHES) + j * (LANES // HASHES) for j in range(HASHES)]

    def prepare(q):
        size_of = jnp.zeros((TILE, LANES), jnp.int32)
        for r in range(TILE):
            size_of = jnp.where(sub8 == r, sizes_ref[q * TILE + r], size_of)
        docs_at = slice(q * TILE, (q + 1) * TILE)
        for e in range(elems // LANES):
            value = elem_ref[docs_at, e * LANES:(e + 1) * LANES]
            value = jnp.where(lane8 + e * LANES < size_of, value, 0.0)
            for p, factor in enumerate(two_factors(value)):
                for j, take in enumerate(takes):
                    at = (e * HASHES + j) * LANES
                    spread[q][2 + p, :, at:at + LANES] = jnp.take_along_axis(factor, take, axis=1)
        for e in range(slots // LANES):
            at = slice(e * LANES, (e + 1) * LANES)
            pos = pos_ref[docs_at, at]
            spread[q][0, :, at] = lax.shift_right_logical(pos, 6).astype(jnp.float32)
            spread[q][1, :, at] = lax.bitwise_and(pos, half - 1).astype(jnp.float32)
        return size_of

    index = lax.broadcasted_iota(jnp.int32, (highs, LANES), 0)
    high_at = 2 * lax.rem(index, lines) + lax.div(index, lines)
    high_at = jnp.concatenate([high_at.astype(jnp.float32).astype(jnp.bfloat16)] * (CHUNK // LANES), axis=1)
    low_at = jnp.concatenate([index.astype(jnp.float32).astype(jnp.bfloat16)] * (CHUNK // LANES), axis=1)
    zero = jnp.zeros((half, CHUNK), jnp.bfloat16)

    def remote(src, dst, send, recv, device):
        return pltpu.make_async_remote_copy(
            src_ref=src, dst_ref=dst, send_sem=send, recv_sem=recv, device_id=device, device_id_type=MESH)

    order = sorted(range(1, blocks), key=lambda k: -min(k, blocks - k))

    def build(q):
        for r in range(TILE):
            total = jnp.zeros((highs, half), jnp.float32)
            for c in range(slots // CHUNK):
                at = slice(c * CHUNK, (c + 1) * CHUNK)

                def row(which):
                    line = jnp.broadcast_to(spread[q][which, r:r + 1, at], (16, CHUNK)).astype(jnp.bfloat16)
                    return jnp.concatenate([line] * (half // 16), axis=0)

                left = jnp.where(row(0) == high_at, row(2), zero)
                right = jnp.where(row(1) == low_at, row(3), zero)
                total = total + lax.dot_general(left, right, NT, preferred_element_type=jnp.float32)
            rows[q][pl.ds(r, lines, stride=TILE), :] = jnp.concatenate([total[:lines], total[lines:]], axis=1)
        pop = jnp.zeros((TILE, LANES), jnp.float32)
        for h in range(lines):
            cells = rows[q][h * TILE:(h + 1) * TILE, :].astype(jnp.bfloat16)
            outbox[q, h * LANES // span, :, h * LANES % span:h * LANES % span + LANES] = cells
            full = cells.astype(jnp.float32)
            weight = bw_ref[h * LANES:(h + 1) * LANES].astype(jnp.float32).reshape(1, LANES)
            pop = pop + (full * weight).astype(jnp.bfloat16).astype(jnp.float32) * full
        pop = jnp.sum(pop, axis=1, keepdims=True)
        return jnp.sum(jnp.where(lane8 == sub8 + q * TILE, pop, 0.0), axis=0, keepdims=True)

    last = near - 1
    line = jnp.zeros((1, LANES), jnp.float32)
    size_of = prepare(0)
    for q in range(near):
        size_now = size_of.astype(jnp.float32)
        if q < last:
            size_of = prepare(q + 1)
        line = line + build(q)
        line = line + jnp.sum(jnp.where(lane8 == sub8 + (q * TILE + docs), size_now, 0.0), axis=0, keepdims=True)
        if q == 0:
            pl.semaphore_wait(barrier, blocks)
        stage = int(q == last)
        for k in order:
            to = shifted(k)
            remote(outbox.at[q, to], slab.at[grp, q, col], send1.at[stage], recv1.at[stage], (to, grp)).start()
        slab[grp, q, col] = outbox[q, col]
    stat_own[...] = line
    for k in order:
        to = shifted(k)
        remote(stat_own, stat.at[grp, col], send1s.at[0], recv1s.at[0], (to, grp)).start()
    stat[grp, col] = stat_own[...]

    spans = (pl.ds(0, last), pl.ds(last, 1))
    news, hands = [], []
    for stage in range(2):
        came = slab.at[grp, spans[stage], pl.ds(0, peers)]
        news.append(remote(outbox.at[spans[stage], pl.ds(0, peers)], came, send1.at[stage], recv1.at[stage], (col, other)))
        news[stage].wait_recv()
        whole = slab.at[grp, spans[stage]]
        hands.append(remote(whole, whole, send2.at[stage], recv2.at[stage], (col, other)))
        hands[stage].start()

    bw = bw_ref[pl.ds(pl.multiple_of(col * span, span), span)].astype(jnp.float32).reshape(1, span)
    share = blocks // groups
    for stage in range(2):
        hands[stage].wait_recv()
        for q in (range(last), [last])[stage]:
            for o in range(share):
                for g in range(groups):
                    value = slab[g, q, grp * share + o].astype(jnp.float32) * bw
                    weighted[(o * groups + g) * near + q] = value.astype(jnp.bfloat16).astype(jnp.float32)

    def multiply(block):
        tiles = [weighted[cand_ref[0, block, c]] for c in range(picks)]
        lines_in = jnp.concatenate(tiles, axis=0).astype(jnp.bfloat16)
        columns = jnp.concatenate([slab[g, q, block] for g in range(groups) for q in range(near)], axis=0)
        return lax.dot_general(columns, lines_in, NT, preferred_element_type=jnp.float32)

    third = []
    to_zero = lax.bitwise_and(blocks - col, blocks - 1)
    for i, k in enumerate(order):
        if i == 0:
            k = jnp.where(col == 0, k, to_zero)
        else:
            k = jnp.where(to_zero == k, order[0], k)
        block = shifted(k)
        part[k] = multiply(block).astype(part.dtype)
        copy = remote(part.at[k], inbox.at[k], send3.at[k], recv3.at[k], (block, grp))
        copy.start()
        third.append(copy)
    shared = multiply(col)

    news_s = remote(stat.at[grp, pl.ds(0, peers)], stat.at[grp, pl.ds(0, peers)], send1s.at[0], recv1s.at[0], (col, other))
    news_s.wait_recv()
    hand_s = remote(stat.at[grp], stat.at[grp], send2s.at[0], recv2s.at[0], (col, other))
    hand_s.start()
    hand_s.wait_recv()

    pop_rows = jnp.zeros((TILE, LANES), jnp.float32)
    size_rows = jnp.zeros((TILE, LANES), jnp.float32)
    for c in range(picks):
        tile = cand_ref[0, col, c]
        owner = lax.div(tile, near)
        line = stat[lax.rem(owner, groups), grp * share + lax.div(owner, groups)]
        spot = lane8 - lax.rem(tile, near) * TILE - sub8
        pop = jnp.sum(jnp.where(spot == 0, line, 0.0), axis=1, keepdims=True)
        size = jnp.sum(jnp.where(spot == docs, line, 0.0), axis=1, keepdims=True)
        here = lane8 == sub8 + c * TILE
        pop_rows = jnp.where(here, pop, pop_rows)
        size_rows = jnp.where(here, size, size_rows)
    pop_rows = jnp.sum(pop_rows, axis=0, keepdims=True)
    size_rows = jnp.sum(size_rows, axis=0, keepdims=True)
    mine = [stat[g, col] for g in range(groups)]
    pop_cols = jnp.concatenate(
        [jnp.sum(jnp.where(lane == sub, line, 0.0), axis=1, keepdims=True) for line in mine], axis=0)
    size_cols = jnp.concatenate(
        [jnp.sum(jnp.where(lane == sub + docs, line, 0.0), axis=1, keepdims=True) for line in mine], axis=0)

    for k in order[::-1]:
        remote(part.at[k], inbox.at[k], send3.at[k], recv3.at[k], (shifted(k), grp)).wait_recv()
        shared = shared + inbox[k].astype(jnp.float32)
    ratio = shared / (pop_rows + pop_cols - shared)
    out_ref[...] = ratio * (size_rows + size_cols) / ((1.0 + ratio) * jnp.minimum(size_rows, size_cols))
    for copy in third + news + hands + [news_s, hand_s]:
        copy.wait_send()


def fast_body(blocks, groups, positions, element_weights, set_sizes, bit_weights, candidates):
    docs, slots = positions.shape
    span = FILTER_BITS // blocks
    near = docs // TILE
    width, rows = docs * groups, candidates.shape[2] * TILE
    vmem, smem = pl.BlockSpec(memory_space=pltpu.VMEM), pl.BlockSpec(memory_space=pltpu.SMEM)
    sems = pltpu.SemaphoreType.DMA
    scores = pl.pallas_call(
        functools.partial(fused_kernel, blocks, groups),
        out_shape=jax.ShapeDtypeStruct((width, rows), jnp.float32),
        in_specs=[smem, smem, vmem, vmem, vmem],
        out_specs=vmem,
        scratch_shapes=[
            [pltpu.VMEM((4, TILE, slots), jnp.float32) for _ in range(near)],
            [pltpu.VMEM((FILTER_BITS // LANES * TILE, LANES), jnp.float32) for _ in range(near)],
            pltpu.VMEM((near, blocks, TILE, span), jnp.bfloat16),
            pltpu.VMEM((1, LANES), jnp.float32),
            pltpu.VMEM((groups, near, blocks, TILE, span), jnp.bfloat16),
            pltpu.VMEM((groups, blocks, 1, LANES), jnp.float32),
            pltpu.VMEM((docs * blocks // TILE, TILE, span), jnp.float32),
            pltpu.VMEM((blocks, width, rows), jnp.bfloat16),
            pltpu.VMEM((blocks, width, rows), jnp.bfloat16),
            sems((2,)), sems((2,)), sems((1,)), sems((1,)), sems((2,)), sems((2,)), sems((1,)), sems((1,)),
            sems((blocks,)), sems((blocks,)),
        ],
        compiler_params=pltpu.CompilerParams(collective_id=0, has_side_effects=True),
    )(candidates, set_sizes, positions, element_weights, bit_weights)
    return scores.T.reshape(1, 1, rows, width)


def solution(mesh):
    blocks, groups = mesh.shape["bits"], mesh.shape["docs"]
    fits = groups == 2 and FILTER_BITS % (blocks * LANES) == 0
    chosen = functools.partial(fast_body, blocks, groups) if fits else body
    return jax.shard_map(
        chosen,
        mesh=mesh,
        in_specs=(
            P(("bits", "docs"), None),
            P(("bits", "docs"), None),
            P(("bits", "docs")),
            P(),
            P("docs", None, None),
        ),
        out_specs=P("docs", "bits", None, None),
        check_vma=False,
    )
```

```python
import functools
import math

import jax
import jax.numpy as jnp
from jax import lax
from jax.experimental import pallas as pl
from jax.experimental.pallas import tpu as pltpu
from jax.sharding import PartitionSpec as P

FILTER_BITS = 4096
HASHES = 4
TILE = 8
LANES = 128
CHUNK = 512
NEAR_LOW = 4
STEPS = (0, 127, 126, 3, 122, 6, 125, 8)
MESH = pl.DeviceIdType.MESH


def build_filter(positions, element_weights, set_sizes):
    doc_count, slot_count = positions.shape
    elem_count = element_weights.shape[1]
    low_cells = 64
    high_cells = FILTER_BITS // low_cells
    slot_index = jnp.arange(slot_count, dtype=jnp.int32)
    usable = slot_index[None, :] < HASHES * set_sizes[:, None]
    spread = jnp.broadcast_to(element_weights[:, :, None], (doc_count, elem_count, HASHES)).reshape(
        doc_count, slot_count
    )
    slot_weights = jnp.where(usable, spread, 0.0)
    upper = slot_weights.astype(jnp.bfloat16)
    remain = slot_weights - upper.astype(jnp.float32)
    middle = remain.astype(jnp.bfloat16)
    lower = (remain - middle.astype(jnp.float32)).astype(jnp.bfloat16)
    weight_parts = jnp.stack([upper, middle, lower], axis=1)
    high_index = positions // low_cells
    low_index = positions - high_index * low_cells
    group = math.gcd(doc_count, 8)

    def one_group(inputs):
        part_block, high_block, low_block = inputs
        high_onehot = (high_block[:, :, None] == jnp.arange(high_cells, dtype=jnp.int32)).astype(
            jnp.bfloat16
        )
        low_onehot = (low_block[:, :, None] == jnp.arange(low_cells, dtype=jnp.int32)).astype(
            jnp.bfloat16
        )
        left = part_block[:, :, :, None] * high_onehot[:, None, :, :]
        summed = jnp.einsum("dcph,dpl->dhl", left, low_onehot, preferred_element_type=jnp.float32)
        return summed.reshape(group, FILTER_BITS)

    grouped = lax.map(
        one_group,
        (
            weight_parts.reshape(doc_count // group, group, 3, slot_count),
            high_index.reshape(doc_count // group, group, slot_count),
            low_index.reshape(doc_count // group, group, slot_count),
        ),
    )
    return grouped.reshape(doc_count, FILTER_BITS).astype(jnp.bfloat16)


def weighted_pop(cells, weights):
    weighted = cells * weights
    return jnp.sum(weighted.astype(jnp.float32) * cells.astype(jnp.float32), axis=1)


def estimate(shared, pop_rows, pop_cols, size_rows, size_cols):
    union_weight = pop_rows[:, None] + pop_cols[None, :] - shared
    ratio = shared / union_weight
    smaller = jnp.minimum(size_rows[:, None], size_cols[None, :])
    return ratio * (size_rows[:, None] + size_cols[None, :]) / ((1.0 + ratio) * smaller)


def pick_tiles(slice_cells, tile_choice, row_group, groups, row_half):
    width = slice_cells.shape[1]
    row_tiles = row_half // TILE
    tiles = slice_cells.reshape(groups, row_tiles, TILE * width)
    own_tiles = lax.dynamic_index_in_dim(tiles, row_group, 0, keepdims=False)
    onehot = (tile_choice[:, :, None] == jnp.arange(row_tiles, dtype=jnp.int32)).astype(
        jnp.bfloat16
    )
    picked = jnp.einsum("jcr,rw->jcw", onehot, own_tiles, preferred_element_type=jnp.float32)
    return picked.astype(jnp.bfloat16).reshape(
        tile_choice.shape[0], tile_choice.shape[1] * TILE, width
    )


def body(positions, element_weights, set_sizes, bit_weights, candidates):
    col_index = lax.axis_index("bits")
    row_group = lax.axis_index("docs")
    blocks = lax.axis_size("bits")
    groups = lax.axis_size("docs")
    doc_total = positions.shape[0] * blocks * groups
    row_half = doc_total // groups
    col_width = doc_total // blocks
    slot_count = candidates.shape[2] * TILE
    tile_offsets = jnp.arange(TILE, dtype=jnp.int32)
    own_cells = build_filter(positions, element_weights, set_sizes)
    local_pop = weighted_pop(own_cells, bit_weights)
    every_pop, size_float = (
        lax.all_gather(local_pop, ("bits", "docs"), axis=0, tiled=True),
        lax.all_gather(set_sizes.astype(jnp.float32), ("bits", "docs"), axis=0, tiled=True),
    )
    pair_cells = lax.all_gather(own_cells, "docs", axis=0, tiled=True)
    slice_cells = lax.all_to_all(pair_cells, "bits", split_axis=1, concat_axis=0, tiled=True)
    tile_rows = row_group * row_half + (candidates[0][:, :, None] * TILE + tile_offsets).reshape(
        blocks, slot_count
    )
    picked_cells = pick_tiles(slice_cells, candidates[0], row_group, groups, row_half)
    row_cells = lax.all_to_all(picked_cells, "bits", split_axis=0, concat_axis=2, tiled=True)[0]
    shared = lax.dot_general(
        row_cells * bit_weights,
        pair_cells,
        (((1,), (1,)), ((), ())),
        preferred_element_type=jnp.float32,
    )
    row_docs = lax.dynamic_index_in_dim(tile_rows, col_index, 0, keepdims=False)
    pop_rows = every_pop[row_docs]
    pop_cols = lax.dynamic_slice_in_dim(every_pop, col_index * col_width, col_width, 0)
    size_rows = size_float[row_docs]
    size_cols = lax.dynamic_slice_in_dim(size_float, col_index * col_width, col_width, 0)
    scores = estimate(shared, pop_rows, pop_cols, size_rows, size_cols)
    return scores.reshape(1, 1, slot_count, col_width)


NT = (((1,), (1,)), ((), ()))


def two_factors(value):
    best_a = value.astype(jnp.bfloat16).astype(jnp.float32)
    best_b = jnp.ones_like(value)
    best_e = jnp.abs(best_a - value)
    for step in STEPS[1:]:
        b = 1.0 + step / 128.0
        a = (value * (1.0 / b)).astype(jnp.bfloat16).astype(jnp.float32)
        e = jnp.abs(a * b - value)
        better = e < best_e
        best_a = jnp.where(better, a, best_a)
        best_b = jnp.where(better, b, best_b)
        best_e = jnp.where(better, e, best_e)
    return best_a, best_b


def fused_kernel(blocks, groups, cand_ref, sizes_ref, pos_ref, elem_ref, bw_ref, out_ref,
                 spread, rows, outbox, stat_own, slab, stat, weighted, part, inbox,
                 send1, recv1, send1s, recv1s, send2, recv2, send2s, recv2s, send3, recv3):
    col, grp = lax.axis_index("bits"), lax.axis_index("docs")
    docs, slots = pos_ref.shape
    elems = elem_ref.shape[1]
    span = slab.shape[4]
    picks = cand_ref.shape[2]
    near = docs // TILE
    other = 1 - grp
    half = LANES // 2
    highs = FILTER_BITS // half
    lines = FILTER_BITS // LANES
    peers = blocks - 1

    low = min(blocks, NEAR_LOW) - 1

    def shifted(k):
        k = jnp.int32(k)
        upper = lax.bitwise_and(lax.bitwise_and(col, blocks - 1 - low) + lax.bitwise_and(k, blocks - 1 - low), blocks - 1)
        return lax.bitwise_or(upper, lax.bitwise_xor(lax.bitwise_and(col, low), lax.bitwise_and(k, low)))

    barrier = pltpu.get_barrier_semaphore()
    for k in range(1, blocks):
        pl.semaphore_signal(barrier, inc=1, device_id=(shifted(k), grp), device_id_type=MESH)
    pl.semaphore_signal(barrier, inc=1, device_id=(col, other), device_id_type=MESH)

    lane = lax.broadcasted_iota(jnp.int32, (docs, LANES), 1)
    sub = lax.broadcasted_iota(jnp.int32, (docs, LANES), 0)
    lane8, sub8 = lane[:TILE], sub[:TILE]
    takes = [lax.div(lane8, HASHES) + j * (LANES // HASHES) for j in range(HASHES)]

    def prepare(q):
        size_of = jnp.zeros((TILE, LANES), jnp.int32)
        for r in range(TILE):
            size_of = jnp.where(sub8 == r, sizes_ref[q * TILE + r], size_of)
        docs_at = slice(q * TILE, (q + 1) * TILE)
        for e in range(elems // LANES):
            value = elem_ref[docs_at, e * LANES:(e + 1) * LANES]
            value = jnp.where(lane8 + e * LANES < size_of, value, 0.0)
            for p, factor in enumerate(two_factors(value)):
                for j, take in enumerate(takes):
                    at = (e * HASHES + j) * LANES
                    spread[q][2 + p, :, at:at + LANES] = jnp.take_along_axis(factor, take, axis=1)
        for e in range(slots // LANES):
            at = slice(e * LANES, (e + 1) * LANES)
            pos = pos_ref[docs_at, at]
            spread[q][0, :, at] = lax.shift_right_logical(pos, 6).astype(jnp.float32)
            spread[q][1, :, at] = lax.bitwise_and(pos, half - 1).astype(jnp.float32)
        return size_of

    index = lax.broadcasted_iota(jnp.int32, (highs, LANES), 0)
    high_at = 2 * lax.rem(index, lines) + lax.div(index, lines)
    high_at = jnp.concatenate([high_at.astype(jnp.float32).astype(jnp.bfloat16)] * (CHUNK // LANES), axis=1)
    low_at = jnp.concatenate([index.astype(jnp.float32).astype(jnp.bfloat16)] * (CHUNK // LANES), axis=1)
    zero = jnp.zeros((half, CHUNK), jnp.bfloat16)

    def remote(src, dst, send, recv, device):
        return pltpu.make_async_remote_copy(
            src_ref=src, dst_ref=dst, send_sem=send, recv_sem=recv, device_id=device, device_id_type=MESH)

    steps = blocks // (low + 1)
    hops = lambda k: min(k // (low + 1), steps - k // (low + 1)) + bin(k & low).count("1")
    order = sorted(range(1, blocks), key=lambda k: (-hops(k), k))

    def build(q):
        for r in range(TILE):
            total = jnp.zeros((highs, half), jnp.float32)
            for c in range(slots // CHUNK):
                at = slice(c * CHUNK, (c + 1) * CHUNK)

                def row(which):
                    line = jnp.broadcast_to(spread[q][which, r:r + 1, at], (16, CHUNK)).astype(jnp.bfloat16)
                    return jnp.concatenate([line] * (half // 16), axis=0)

                left = jnp.where(row(0) == high_at, row(2), zero)
                right = jnp.where(row(1) == low_at, row(3), zero)
                total = total + lax.dot_general(left, right, NT, preferred_element_type=jnp.float32)
            rows[q][pl.ds(r, lines, stride=TILE), :] = jnp.concatenate([total[:lines], total[lines:]], axis=1)
        pop = jnp.zeros((TILE, LANES), jnp.float32)
        for h in range(lines):
            cells = rows[q][h * TILE:(h + 1) * TILE, :].astype(jnp.bfloat16)
            outbox[q, h * LANES // span, :, h * LANES % span:h * LANES % span + LANES] = cells
            full = cells.astype(jnp.float32)
            weight = bw_ref[h * LANES:(h + 1) * LANES].astype(jnp.float32).reshape(1, LANES)
            pop = pop + (full * weight).astype(jnp.bfloat16).astype(jnp.float32) * full
        pop = jnp.sum(pop, axis=1, keepdims=True)
        return jnp.sum(jnp.where(lane8 == sub8 + q * TILE, pop, 0.0), axis=0, keepdims=True)

    last = near - 1
    line = jnp.zeros((1, LANES), jnp.float32)
    size_of = prepare(0)
    for q in range(near):
        size_now = size_of.astype(jnp.float32)
        if q < last:
            size_of = prepare(q + 1)
        line = line + build(q)
        line = line + jnp.sum(jnp.where(lane8 == sub8 + (q * TILE + docs), size_now, 0.0), axis=0, keepdims=True)
        slab[grp, q, col] = outbox[q, col]
        if q == 0:
            continue
        if q == 1:
            pl.semaphore_wait(barrier, blocks)
        stage = int(q == last)
        for s in ((0, 1) if q == 1 else (q,)):
            for k in order:
                to = shifted(k)
                remote(outbox.at[s, to], slab.at[grp, s, col], send1.at[stage], recv1.at[stage], (to, grp)).start()
    stat_own[...] = line
    for k in order:
        to = shifted(k)
        remote(stat_own, stat.at[grp, col], send1s.at[0], recv1s.at[0], (to, grp)).start()
    stat[grp, col] = stat_own[...]

    spans = (pl.ds(0, last), pl.ds(last, 1))
    news, hands = [], []
    for stage in range(2):
        came = slab.at[grp, spans[stage], pl.ds(0, peers)]
        news.append(remote(outbox.at[spans[stage], pl.ds(0, peers)], came, send1.at[stage], recv1.at[stage], (col, other)))
        news[stage].wait_recv()
        whole = slab.at[grp, spans[stage]]
        hands.append(remote(whole, whole, send2.at[stage], recv2.at[stage], (col, other)))
        hands[stage].start()

    bw = bw_ref[pl.ds(pl.multiple_of(col * span, span), span)].astype(jnp.float32).reshape(1, span)
    share = blocks // groups
    for stage in range(2):
        hands[stage].wait_recv()
        for q in (range(last), [last])[stage]:
            for o in range(share):
                for g in range(groups):
                    value = slab[g, q, grp * share + o].astype(jnp.float32) * bw
                    weighted[(o * groups + g) * near + q] = value.astype(jnp.bfloat16).astype(jnp.float32)

    def multiply(block):
        tiles = [weighted[cand_ref[0, block, c]] for c in range(picks)]
        lines_in = jnp.concatenate(tiles, axis=0).astype(jnp.bfloat16)
        columns = jnp.concatenate([slab[g, q, block] for g in range(groups) for q in range(near)], axis=0)
        return lax.dot_general(columns, lines_in, NT, preferred_element_type=jnp.float32)

    third = []
    to_zero = lax.bitwise_or(lax.bitwise_and(blocks - lax.bitwise_and(col, blocks - 1 - low), blocks - 1),
                             lax.bitwise_and(col, low))
    for i, k in enumerate(order):
        if i == 0:
            k = jnp.where(col == 0, k, to_zero)
        else:
            k = jnp.where(to_zero == k, order[0], k)
        block = shifted(k)
        part[k] = multiply(block).astype(part.dtype)
        copy = remote(part.at[k], inbox.at[k], send3.at[k], recv3.at[k], (block, grp))
        copy.start()
        third.append(copy)
    shared = multiply(col)

    news_s = remote(stat.at[grp, pl.ds(0, peers)], stat.at[grp, pl.ds(0, peers)], send1s.at[0], recv1s.at[0], (col, other))
    news_s.wait_recv()
    hand_s = remote(stat.at[grp], stat.at[grp], send2s.at[0], recv2s.at[0], (col, other))
    hand_s.start()
    hand_s.wait_recv()

    pop_rows = jnp.zeros((TILE, LANES), jnp.float32)
    size_rows = jnp.zeros((TILE, LANES), jnp.float32)
    for c in range(picks):
        tile = cand_ref[0, col, c]
        owner = lax.div(tile, near)
        line = stat[lax.rem(owner, groups), grp * share + lax.div(owner, groups)]
        spot = lane8 - lax.rem(tile, near) * TILE - sub8
        pop = jnp.sum(jnp.where(spot == 0, line, 0.0), axis=1, keepdims=True)
        size = jnp.sum(jnp.where(spot == docs, line, 0.0), axis=1, keepdims=True)
        here = lane8 == sub8 + c * TILE
        pop_rows = jnp.where(here, pop, pop_rows)
        size_rows = jnp.where(here, size, size_rows)
    pop_rows = jnp.sum(pop_rows, axis=0, keepdims=True)
    size_rows = jnp.sum(size_rows, axis=0, keepdims=True)
    mine = [stat[g, col] for g in range(groups)]
    pop_cols = jnp.concatenate(
        [jnp.sum(jnp.where(lane == sub, line, 0.0), axis=1, keepdims=True) for line in mine], axis=0)
    size_cols = jnp.concatenate(
        [jnp.sum(jnp.where(lane == sub + docs, line, 0.0), axis=1, keepdims=True) for line in mine], axis=0)

    for k in order[::-1]:
        remote(part.at[k], inbox.at[k], send3.at[k], recv3.at[k], (shifted(k), grp)).wait_recv()
        shared = shared + inbox[k].astype(jnp.float32)
    ratio = shared / (pop_rows + pop_cols - shared)
    out_ref[...] = ratio * (size_rows + size_cols) / ((1.0 + ratio) * jnp.minimum(size_rows, size_cols))
    for copy in third + news + hands + [news_s, hand_s]:
        copy.wait_send()


def fast_body(blocks, groups, positions, element_weights, set_sizes, bit_weights, candidates):
    docs, slots = positions.shape
    span = FILTER_BITS // blocks
    near = docs // TILE
    width, rows = docs * groups, candidates.shape[2] * TILE
    vmem, smem = pl.BlockSpec(memory_space=pltpu.VMEM), pl.BlockSpec(memory_space=pltpu.SMEM)
    sems = pltpu.SemaphoreType.DMA
    scores = pl.pallas_call(
        functools.partial(fused_kernel, blocks, groups),
        out_shape=pltpu.VMEM((width, rows), jnp.float32),
        in_specs=[smem, smem, vmem, vmem, vmem],
        out_specs=vmem,
        scratch_shapes=[
            [pltpu.VMEM((4, TILE, slots), jnp.float32) for _ in range(near)],
            [pltpu.VMEM((FILTER_BITS // LANES * TILE, LANES), jnp.float32) for _ in range(near)],
            pltpu.VMEM((near, blocks, TILE, span), jnp.bfloat16),
            pltpu.VMEM((1, LANES), jnp.float32),
            pltpu.VMEM((groups, near, blocks, TILE, span), jnp.bfloat16),
            pltpu.VMEM((groups, blocks, 1, LANES), jnp.float32),
            pltpu.VMEM((docs * blocks // TILE, TILE, span), jnp.float32),
            pltpu.VMEM((blocks, width, rows), jnp.bfloat16),
            pltpu.VMEM((blocks, width, rows), jnp.bfloat16),
            sems((2,)), sems((2,)), sems((1,)), sems((1,)), sems((2,)), sems((2,)), sems((1,)), sems((1,)),
            sems((blocks,)), sems((blocks,)),
        ],
        compiler_params=pltpu.CompilerParams(collective_id=0, has_side_effects=True),
    )(candidates, set_sizes, positions, element_weights, bit_weights)
    return scores.T.reshape(1, 1, rows, width)


def solution(mesh):
    blocks, groups = mesh.shape["bits"], mesh.shape["docs"]
    fits = groups == 2 and FILTER_BITS % (blocks * LANES) == 0
    chosen = functools.partial(fast_body, blocks, groups) if fits else body
    return jax.shard_map(
        chosen,
        mesh=mesh,
        in_specs=(
            P(("bits", "docs"), None),
            P(("bits", "docs"), None),
            P(("bits", "docs")),
            P(),
            P("docs", None, None),
        ),
        out_specs=P("docs", "bits", None, None),
        check_vma=False,
    )
```

```python
import functools
import math

import jax
import jax.numpy as jnp
from jax import lax
from jax.experimental import pallas as pl
from jax.experimental.pallas import tpu as pltpu
from jax.sharding import PartitionSpec as P

FILTER_BITS = 4096
HASHES = 4
TILE = 8
LANES = 128
CHUNK = 512
NEAR_LOW = 4
STEPS = (0, 127, 126, 3, 122, 6, 125, 8)
MESH = pl.DeviceIdType.MESH


def build_filter(positions, element_weights, set_sizes):
    doc_count, slot_count = positions.shape
    elem_count = element_weights.shape[1]
    low_cells = 64
    high_cells = FILTER_BITS // low_cells
    slot_index = jnp.arange(slot_count, dtype=jnp.int32)
    usable = slot_index[None, :] < HASHES * set_sizes[:, None]
    spread = jnp.broadcast_to(element_weights[:, :, None], (doc_count, elem_count, HASHES)).reshape(
        doc_count, slot_count
    )
    slot_weights = jnp.where(usable, spread, 0.0)
    upper = slot_weights.astype(jnp.bfloat16)
    remain = slot_weights - upper.astype(jnp.float32)
    middle = remain.astype(jnp.bfloat16)
    lower = (remain - middle.astype(jnp.float32)).astype(jnp.bfloat16)
    weight_parts = jnp.stack([upper, middle, lower], axis=1)
    high_index = positions // low_cells
    low_index = positions - high_index * low_cells
    group = math.gcd(doc_count, 8)

    def one_group(inputs):
        part_block, high_block, low_block = inputs
        high_onehot = (high_block[:, :, None] == jnp.arange(high_cells, dtype=jnp.int32)).astype(
            jnp.bfloat16
        )
        low_onehot = (low_block[:, :, None] == jnp.arange(low_cells, dtype=jnp.int32)).astype(
            jnp.bfloat16
        )
        left = part_block[:, :, :, None] * high_onehot[:, None, :, :]
        summed = jnp.einsum("dcph,dpl->dhl", left, low_onehot, preferred_element_type=jnp.float32)
        return summed.reshape(group, FILTER_BITS)

    grouped = lax.map(
        one_group,
        (
            weight_parts.reshape(doc_count // group, group, 3, slot_count),
            high_index.reshape(doc_count // group, group, slot_count),
            low_index.reshape(doc_count // group, group, slot_count),
        ),
    )
    return grouped.reshape(doc_count, FILTER_BITS).astype(jnp.bfloat16)


def weighted_pop(cells, weights):
    weighted = cells * weights
    return jnp.sum(weighted.astype(jnp.float32) * cells.astype(jnp.float32), axis=1)


def estimate(shared, pop_rows, pop_cols, size_rows, size_cols):
    union_weight = pop_rows[:, None] + pop_cols[None, :] - shared
    ratio = shared / union_weight
    smaller = jnp.minimum(size_rows[:, None], size_cols[None, :])
    return ratio * (size_rows[:, None] + size_cols[None, :]) / ((1.0 + ratio) * smaller)


def pick_tiles(slice_cells, tile_choice, row_group, groups, row_half):
    width = slice_cells.shape[1]
    row_tiles = row_half // TILE
    tiles = slice_cells.reshape(groups, row_tiles, TILE * width)
    own_tiles = lax.dynamic_index_in_dim(tiles, row_group, 0, keepdims=False)
    onehot = (tile_choice[:, :, None] == jnp.arange(row_tiles, dtype=jnp.int32)).astype(
        jnp.bfloat16
    )
    picked = jnp.einsum("jcr,rw->jcw", onehot, own_tiles, preferred_element_type=jnp.float32)
    return picked.astype(jnp.bfloat16).reshape(
        tile_choice.shape[0], tile_choice.shape[1] * TILE, width
    )


def body(positions, element_weights, set_sizes, bit_weights, candidates):
    col_index = lax.axis_index("bits")
    row_group = lax.axis_index("docs")
    blocks = lax.axis_size("bits")
    groups = lax.axis_size("docs")
    doc_total = positions.shape[0] * blocks * groups
    row_half = doc_total // groups
    col_width = doc_total // blocks
    slot_count = candidates.shape[2] * TILE
    tile_offsets = jnp.arange(TILE, dtype=jnp.int32)
    own_cells = build_filter(positions, element_weights, set_sizes)
    local_pop = weighted_pop(own_cells, bit_weights)
    every_pop, size_float = (
        lax.all_gather(local_pop, ("bits", "docs"), axis=0, tiled=True),
        lax.all_gather(set_sizes.astype(jnp.float32), ("bits", "docs"), axis=0, tiled=True),
    )
    pair_cells = lax.all_gather(own_cells, "docs", axis=0, tiled=True)
    slice_cells = lax.all_to_all(pair_cells, "bits", split_axis=1, concat_axis=0, tiled=True)
    tile_rows = row_group * row_half + (candidates[0][:, :, None] * TILE + tile_offsets).reshape(
        blocks, slot_count
    )
    picked_cells = pick_tiles(slice_cells, candidates[0], row_group, groups, row_half)
    row_cells = lax.all_to_all(picked_cells, "bits", split_axis=0, concat_axis=2, tiled=True)[0]
    shared = lax.dot_general(
        row_cells * bit_weights,
        pair_cells,
        (((1,), (1,)), ((), ())),
        preferred_element_type=jnp.float32,
    )
    row_docs = lax.dynamic_index_in_dim(tile_rows, col_index, 0, keepdims=False)
    pop_rows = every_pop[row_docs]
    pop_cols = lax.dynamic_slice_in_dim(every_pop, col_index * col_width, col_width, 0)
    size_rows = size_float[row_docs]
    size_cols = lax.dynamic_slice_in_dim(size_float, col_index * col_width, col_width, 0)
    scores = estimate(shared, pop_rows, pop_cols, size_rows, size_cols)
    return scores.reshape(1, 1, slot_count, col_width)


NT = (((1,), (1,)), ((), ()))


def two_factors(value):
    best_a = value.astype(jnp.bfloat16).astype(jnp.float32)
    best_b = jnp.ones_like(value)
    best_e = jnp.abs(best_a - value)
    for step in STEPS[1:]:
        b = 1.0 + step / 128.0
        a = (value * (1.0 / b)).astype(jnp.bfloat16).astype(jnp.float32)
        e = jnp.abs(a * b - value)
        better = e < best_e
        best_a = jnp.where(better, a, best_a)
        best_b = jnp.where(better, b, best_b)
        best_e = jnp.where(better, e, best_e)
    return best_a, best_b


def fused_kernel(blocks, groups, cand_ref, sizes_ref, pos_ref, elem_ref, bw_ref, out_ref,
                 spread, rows, outbox, stat_own, slab, stat, weighted, part, inbox,
                 send1, recv1, send1s, recv1s, send2, recv2, send2s, recv2s, send3, recv3):
    col, grp = lax.axis_index("bits"), lax.axis_index("docs")
    docs, slots = pos_ref.shape
    elems = elem_ref.shape[1]
    span = slab.shape[4]
    picks = cand_ref.shape[2]
    near = docs // TILE
    other = 1 - grp
    half = LANES // 2
    highs = FILTER_BITS // half
    lines = FILTER_BITS // LANES
    peers = blocks - 1

    low = min(blocks, NEAR_LOW) - 1

    def shifted(k):
        k = jnp.int32(k)
        upper = lax.bitwise_and(lax.bitwise_and(col, blocks - 1 - low) + lax.bitwise_and(k, blocks - 1 - low), blocks - 1)
        return lax.bitwise_or(upper, lax.bitwise_xor(lax.bitwise_and(col, low), lax.bitwise_and(k, low)))

    barrier = pltpu.get_barrier_semaphore()
    for k in range(1, blocks):
        pl.semaphore_signal(barrier, inc=1, device_id=(shifted(k), grp), device_id_type=MESH)
    pl.semaphore_signal(barrier, inc=1, device_id=(col, other), device_id_type=MESH)

    lane = lax.broadcasted_iota(jnp.int32, (docs, LANES), 1)
    sub = lax.broadcasted_iota(jnp.int32, (docs, LANES), 0)
    lane8, sub8 = lane[:TILE], sub[:TILE]
    takes = [lax.div(lane8, HASHES) + j * (LANES // HASHES) for j in range(HASHES)]

    def prepare(q):
        size_of = jnp.zeros((TILE, LANES), jnp.int32)
        for r in range(TILE):
            size_of = jnp.where(sub8 == r, sizes_ref[q * TILE + r], size_of)
        docs_at = slice(q * TILE, (q + 1) * TILE)
        for e in range(elems // LANES):
            value = elem_ref[docs_at, e * LANES:(e + 1) * LANES]
            value = jnp.where(lane8 + e * LANES < size_of, value, 0.0)
            for p, factor in enumerate(two_factors(value)):
                for j, take in enumerate(takes):
                    at = (e * HASHES + j) * LANES
                    spread[q][2 + p, :, at:at + LANES] = jnp.take_along_axis(factor, take, axis=1)
        for e in range(slots // LANES):
            at = slice(e * LANES, (e + 1) * LANES)
            pos = pos_ref[docs_at, at]
            spread[q][0, :, at] = lax.shift_right_logical(pos, 6).astype(jnp.float32)
            spread[q][1, :, at] = lax.bitwise_and(pos, half - 1).astype(jnp.float32)
        return size_of

    index = lax.broadcasted_iota(jnp.int32, (highs, LANES), 0)
    high_at = 2 * lax.rem(index, lines) + lax.div(index, lines)
    high_at = jnp.concatenate([high_at.astype(jnp.float32).astype(jnp.bfloat16)] * (CHUNK // LANES), axis=1)
    low_at = jnp.concatenate([index.astype(jnp.float32).astype(jnp.bfloat16)] * (CHUNK // LANES), axis=1)
    zero = jnp.zeros((half, CHUNK), jnp.bfloat16)

    def remote(src, dst, send, recv, device):
        return pltpu.make_async_remote_copy(
            src_ref=src, dst_ref=dst, send_sem=send, recv_sem=recv, device_id=device, device_id_type=MESH)

    steps = blocks // (low + 1)
    hops = lambda k: min(k // (low + 1), steps - k // (low + 1)) + bin(k & low).count("1")
    order = sorted(range(1, blocks), key=lambda k: (-hops(k), k))

    def build(q):
        for r in range(TILE):
            total = jnp.zeros((highs, half), jnp.float32)
            for c in range(slots // CHUNK):
                at = slice(c * CHUNK, (c + 1) * CHUNK)

                def row(which):
                    line = jnp.broadcast_to(spread[q][which, r:r + 1, at], (16, CHUNK)).astype(jnp.bfloat16)
                    return jnp.concatenate([line] * (half // 16), axis=0)

                left = jnp.where(row(0) == high_at, row(2), zero)
                right = jnp.where(row(1) == low_at, row(3), zero)
                total = total + lax.dot_general(left, right, NT, preferred_element_type=jnp.float32)
            rows[q][pl.ds(r, lines, stride=TILE), :] = jnp.concatenate([total[:lines], total[lines:]], axis=1)
        pop = jnp.zeros((TILE, LANES), jnp.float32)
        for h in range(lines):
            cells = rows[q][h * TILE:(h + 1) * TILE, :].astype(jnp.bfloat16)
            outbox[q, h * LANES // span, :, h * LANES % span:h * LANES % span + LANES] = cells
            full = cells.astype(jnp.float32)
            weight = bw_ref[h * LANES:(h + 1) * LANES].astype(jnp.float32).reshape(1, LANES)
            pop = pop + (full * weight).astype(jnp.bfloat16).astype(jnp.float32) * full
        pop = jnp.sum(pop, axis=1, keepdims=True)
        return jnp.sum(jnp.where(lane8 == sub8 + q * TILE, pop, 0.0), axis=0, keepdims=True)

    last = near - 1
    line = jnp.zeros((1, LANES), jnp.float32)
    size_of = prepare(0)
    for q in range(near):
        size_now = size_of.astype(jnp.float32)
        if q < last:
            size_of = prepare(q + 1)
        line = line + build(q)
        line = line + jnp.sum(jnp.where(lane8 == sub8 + (q * TILE + docs), size_now, 0.0), axis=0, keepdims=True)
        slab[grp, q, col] = outbox[q, col]
        if q == 0:
            continue
        if q == 1:
            pl.semaphore_wait(barrier, blocks)
        stage = int(q == last)
        for s in ((0, 1) if q == 1 else (q,)):
            for k in order:
                to = shifted(k)
                remote(outbox.at[s, to], slab.at[grp, s, col], send1.at[stage], recv1.at[stage], (to, grp)).start()
    stat_own[...] = line
    for k in order:
        to = shifted(k)
        remote(stat_own, stat.at[grp, col], send1s.at[0], recv1s.at[0], (to, grp)).start()
    stat[grp, col] = stat_own[...]

    spans = (pl.ds(0, last), pl.ds(last, 1))
    news, hands = [], []
    for stage in range(2):
        came = slab.at[grp, spans[stage], pl.ds(0, peers)]
        news.append(remote(outbox.at[spans[stage], pl.ds(0, peers)], came, send1.at[stage], recv1.at[stage], (col, other)))
        news[stage].wait_recv()
        whole = slab.at[grp, spans[stage]]
        hands.append(remote(whole, whole, send2.at[stage], recv2.at[stage], (col, other)))
        hands[stage].start()

    bw = bw_ref[pl.ds(pl.multiple_of(col * span, span), span)].astype(jnp.float32).reshape(1, span)
    share = blocks // groups
    for stage in range(2):
        hands[stage].wait_recv()
        for q in (range(last), [last])[stage]:
            for o in range(share):
                for g in range(groups):
                    value = slab[g, q, grp * share + o].astype(jnp.float32) * bw
                    weighted[(o * groups + g) * near + q] = value.astype(jnp.bfloat16).astype(jnp.float32)

    def multiply(block):
        tiles = [weighted[cand_ref[0, block, c]] for c in range(picks)]
        lines_in = jnp.concatenate(tiles, axis=0).astype(jnp.bfloat16)
        columns = jnp.concatenate([slab[g, q, block] for g in range(groups) for q in range(near)], axis=0)
        return lax.dot_general(columns, lines_in, NT, preferred_element_type=jnp.float32)

    third = []
    to_zero = lax.bitwise_or(lax.bitwise_and(blocks - lax.bitwise_and(col, blocks - 1 - low), blocks - 1),
                             lax.bitwise_and(col, low))
    late = sorted(order, key=lambda k: (-hops(k), abs(k // (low + 1) - steps // 2), -k))
    for i, k in enumerate(late):
        if i == 0:
            k = jnp.where(col == 0, k, to_zero)
        else:
            k = jnp.where(to_zero == k, late[0], k)
        block = shifted(k)
        part[k] = multiply(block).astype(part.dtype)
        copy = remote(part.at[k], inbox.at[k], send3.at[k], recv3.at[k], (block, grp))
        copy.start()
        third.append(copy)
    shared = multiply(col)

    news_s = remote(stat.at[grp, pl.ds(0, peers)], stat.at[grp, pl.ds(0, peers)], send1s.at[0], recv1s.at[0], (col, other))
    news_s.wait_recv()
    hand_s = remote(stat.at[grp], stat.at[grp], send2s.at[0], recv2s.at[0], (col, other))
    hand_s.start()
    hand_s.wait_recv()

    pop_rows = jnp.zeros((TILE, LANES), jnp.float32)
    size_rows = jnp.zeros((TILE, LANES), jnp.float32)
    for c in range(picks):
        tile = cand_ref[0, col, c]
        owner = lax.div(tile, near)
        line = stat[lax.rem(owner, groups), grp * share + lax.div(owner, groups)]
        spot = lane8 - lax.rem(tile, near) * TILE - sub8
        pop = jnp.sum(jnp.where(spot == 0, line, 0.0), axis=1, keepdims=True)
        size = jnp.sum(jnp.where(spot == docs, line, 0.0), axis=1, keepdims=True)
        here = lane8 == sub8 + c * TILE
        pop_rows = jnp.where(here, pop, pop_rows)
        size_rows = jnp.where(here, size, size_rows)
    pop_rows = jnp.sum(pop_rows, axis=0, keepdims=True)
    size_rows = jnp.sum(size_rows, axis=0, keepdims=True)
    mine = [stat[g, col] for g in range(groups)]
    pop_cols = jnp.concatenate(
        [jnp.sum(jnp.where(lane == sub, line, 0.0), axis=1, keepdims=True) for line in mine], axis=0)
    size_cols = jnp.concatenate(
        [jnp.sum(jnp.where(lane == sub + docs, line, 0.0), axis=1, keepdims=True) for line in mine], axis=0)

    for k in order[::-1]:
        remote(part.at[k], inbox.at[k], send3.at[k], recv3.at[k], (shifted(k), grp)).wait_recv()
        shared = shared + inbox[k].astype(jnp.float32)
    ratio = shared / (pop_rows + pop_cols - shared)
    out_ref[...] = ratio * (size_rows + size_cols) / ((1.0 + ratio) * jnp.minimum(size_rows, size_cols))
    for copy in third + news + hands + [news_s, hand_s]:
        copy.wait_send()


def fast_body(blocks, groups, positions, element_weights, set_sizes, bit_weights, candidates):
    docs, slots = positions.shape
    span = FILTER_BITS // blocks
    near = docs // TILE
    width, rows = docs * groups, candidates.shape[2] * TILE
    vmem, smem = pl.BlockSpec(memory_space=pltpu.VMEM), pl.BlockSpec(memory_space=pltpu.SMEM)
    sems = pltpu.SemaphoreType.DMA
    scores = pl.pallas_call(
        functools.partial(fused_kernel, blocks, groups),
        out_shape=pltpu.VMEM((width, rows), jnp.float32),
        in_specs=[smem, smem, vmem, vmem, vmem],
        out_specs=vmem,
        scratch_shapes=[
            [pltpu.VMEM((4, TILE, slots), jnp.float32) for _ in range(near)],
            [pltpu.VMEM((FILTER_BITS // LANES * TILE, LANES), jnp.float32) for _ in range(near)],
            pltpu.VMEM((near, blocks, TILE, span), jnp.bfloat16),
            pltpu.VMEM((1, LANES), jnp.float32),
            pltpu.VMEM((groups, near, blocks, TILE, span), jnp.bfloat16),
            pltpu.VMEM((groups, blocks, 1, LANES), jnp.float32),
            pltpu.VMEM((docs * blocks // TILE, TILE, span), jnp.float32),
            pltpu.VMEM((blocks, width, rows), jnp.bfloat16),
            pltpu.VMEM((blocks, width, rows), jnp.bfloat16),
            sems((2,)), sems((2,)), sems((1,)), sems((1,)), sems((2,)), sems((2,)), sems((1,)), sems((1,)),
            sems((blocks,)), sems((blocks,)),
        ],
        compiler_params=pltpu.CompilerParams(collective_id=0, has_side_effects=True),
    )(candidates, set_sizes, positions, element_weights, bit_weights)
    return scores.T.reshape(1, 1, rows, width)


def solution(mesh):
    blocks, groups = mesh.shape["bits"], mesh.shape["docs"]
    fits = groups == 2 and FILTER_BITS % (blocks * LANES) == 0
    chosen = functools.partial(fast_body, blocks, groups) if fits else body
    return jax.shard_map(
        chosen,
        mesh=mesh,
        in_specs=(
            P(("bits", "docs"), None),
            P(("bits", "docs"), None),
            P(("bits", "docs")),
            P(),
            P("docs", None, None),
        ),
        out_specs=P("docs", "bits", None, None),
        check_vma=False,
    )
```
